32 devices in a mesh: gx: 4 (over y, x), gy: 8 (over z, core).
Axes of the slice: x: 2, y: 2, z: 4, core: 2. Of those that a mesh axis runs over, the one named last changes fastest.
Arguments:
- e_field: float32 [3, 128, 256, 128], P(None, 'gx', 'gy'), may hold values from -6 to 6
- h_field: float32 [3, 128, 256, 128], P(None, 'gx', 'gy'), may hold values from -6 to 6
- psi: float32 [12, 128, 256, 128], P(None, 'gx', 'gy'), may hold values from -6 to 6
- material: int32 [128, 256, 128], P('gx', 'gy'), may hold values from 0 to 7
- eps_table: float32 [8], replicated, may hold values from 1 to 1.2
- sigma_table: float32 [8], replicated, may hold values from 0 to 0.05
Outputs:
- e_out: float32 [3, 128, 256, 128], P(None, 'gx', 'gy')
- h_out: float32 [3, 128, 256, 128], P(None, 'gx', 'gy')
- psi_out: float32 [12, 128, 256, 128], P(None, 'gx', 'gy')
The draws below stay inside these ranges and needn't reach their ends.
All inputs are finite; a program needn't handle non-finite values.
Results may differ from the reference program's by a relative error of at most 0.0003.
Values sent between devices are 32-bit elements; how exact they have to be, the bound alone decides.
A program may use at most 128 MiB of HBM per device.

```python
import math
import jax
import jax.numpy as jnp
from jax import lax

NZ = 128
PML = 16
STEPS = 16
NMAT = 8
NX = 128
NY = 256


def place_ends(array, stream_key, smallest, high):
    longest = array.shape.index(max(array.shape))
    spots = []
    for shift in (0, 1):
        where = [jax.random.randint(jax.random.fold_in(stream_key, axis), (), 0, length) for axis, length in enumerate(array.shape)]
        where[longest] = (where[longest] + shift) % array.shape[longest]
        spots.append(tuple(where))
    return array.at[spots[0]].set(smallest).at[spots[1]].set(high)


def block_scale(own_key, shape, pieces, least, top_value):
    gain = 1.0
    for dim, parts in pieces:
        heights = jax.random.uniform(jax.random.fold_in(jax.random.fold_in(own_key, 6), dim), (parts,), jnp.float32, least / len(pieces), top_value / len(pieces))
        gain = gain * jnp.repeat(jnp.exp(heights), shape[dim] // parts).reshape((-1,) + (1,) * (len(shape) - 1 - dim))
    return gain


def normal_values(stream_key, dims, spread, reach, cuts=(), kind=jnp.bfloat16):
    result = jax.random.normal(stream_key, dims, jnp.float32) * spread
    if len(cuts) > 0:
        result = block_scale(stream_key, dims, cuts, -0.22, 0.18) * result
    return jnp.clip(result, min=-reach, max=reach).astype(kind)


def setup_inputs(seed: int = 0) -> dict:
    seeds = jax.random.split(jax.random.key(seed), 7)
    e_field = normal_values(seeds[0], (3, NX, NY, NZ), 1.0, 6.0, ((1, 4), (2, 8)), jnp.float32)
    h_field = normal_values(seeds[1], (3, NX, NY, NZ), 1.0, 6.0, ((1, 4), (2, 8)), jnp.float32)
    psi = normal_values(seeds[2], (12, NX, NY, NZ), 1.0, 6.0, ((1, 4), (2, 8)), jnp.float32)
    material = place_ends(jax.random.randint(seeds[3], (NX, NY, NZ), 0, NMAT), jax.random.fold_in(seeds[3], 1), 0, NMAT - 1).astype(jnp.int32)
    eps_table = jnp.clip(jnp.exp(jax.random.uniform(seeds[4], (NMAT,), jnp.float32, math.log(1.0), math.log(1.2))), 1.0, 1.2)
    sigma_table = jnp.clip(jax.random.uniform(seeds[5], (NMAT,), jnp.float32, 0.0, 0.05), 0.0, 0.05)
    return {"e_field": e_field, "h_field": h_field, "psi": psi, "material": material, "eps_table": eps_table, "sigma_table": sigma_table}


time_step = 0.5
sigma_peak = 3.0
kappa_peak = 5.0
alpha_peak = 0.05
curl_table = (((2, 1), (1, 2)), ((0, 2), (2, 0)), ((1, 0), (0, 1)))


def profile(length, offset, extent, shift_half, thickness):
    position = (offset + lax.iota(jnp.int32, length)).astype(jnp.float32) + shift_half
    slab_width = jnp.float32(thickness)
    depth_frac = jnp.maximum(jnp.maximum((slab_width - position) / slab_width, (position - (extent - slab_width)) / slab_width), 0.0)
    depth_cube = depth_frac * depth_frac * depth_frac
    sigma_value = sigma_peak * depth_cube
    kappa_value = 1.0 + (kappa_peak - 1.0) * depth_cube
    alpha_value = alpha_peak * (1.0 - depth_frac)
    decays = jnp.exp(-(sigma_value / kappa_value + alpha_value) * time_step)
    scaling = sigma_value * (decays - 1.0) / (kappa_value * (sigma_value + kappa_value * alpha_value))
    inside_slab = depth_frac > 0.0
    return jnp.where(inside_slab, decays, 0.0), jnp.where(inside_slab, scaling, 0.0), 1.0 / kappa_value


def shaped(vector, direction):
    target_shape = [1, 1, 1]
    target_shape[direction] = vector.shape[0]
    return vector.reshape(target_shape)


def forward(field, direction, following):
    shifted = lax.slice_in_dim(field, 1, field.shape[direction], axis=direction)
    return jnp.concatenate([shifted, following], axis=direction) - field


def backward(field, direction, preceding):
    shifted = lax.slice_in_dim(field, 0, field.shape[direction] - 1, axis=direction)
    return field - jnp.concatenate([preceding, shifted], axis=direction)


def zero_layer(field, direction):
    return jnp.zeros_like(lax.slice_in_dim(field, 0, 1, axis=direction))


def update_term(difference, auxiliary, coefficient, direction):
    decays, scaling, inverse = coefficient
    renewed = decays * auxiliary + scaling * difference
    return inverse * difference + renewed, renewed


def curl(difference_of, auxiliary, first_slot, coefficients, renew):
    results = []
    renewed_list = []
    for component in range(3):
        plus_pair, minus_pair = curl_table[component]
        slot = first_slot + 2 * component
        plus_value, plus_aux = renew(difference_of(plus_pair[0], plus_pair[1]), auxiliary[slot], coefficients[plus_pair[1]], plus_pair[1])
        minus_value, minus_aux = renew(difference_of(minus_pair[0], minus_pair[1]), auxiliary[slot + 1], coefficients[minus_pair[1]], minus_pair[1])
        results.append(plus_value - minus_value)
        renewed_list.append(plus_aux)
        renewed_list.append(minus_aux)
    return results, renewed_list


def material_coefficients(material, eps_table, sigma_table):
    losses = sigma_table * time_step / (2.0 * eps_table)
    keep_table = (1.0 - losses) / (1.0 + losses)
    drive_table = (time_step / eps_table) / (1.0 + losses)
    keeping = jnp.zeros(material.shape, jnp.float32)
    driving = jnp.zeros(material.shape, jnp.float32)
    for number in range(NMAT):
        chosen = material == number
        keeping = keeping + jnp.where(chosen, keep_table[number], 0.0)
        driving = driving + jnp.where(chosen, drive_table[number], 0.0)
    return keeping, driving


def reference(e_field, h_field, psi, material, eps_table, sigma_table):
    extents = (NX, NY, NZ)
    magnetic_coef = [tuple(shaped(vector, direction) for vector in profile(extents[direction], 0, extents[direction], 0.5, PML)) for direction in range(3)]
    electric_coef = [tuple(shaped(vector, direction) for vector in profile(extents[direction], 0, extents[direction], 0.0, PML)) for direction in range(3)]
    keeping, driving = material_coefficients(material, eps_table, sigma_table)

    def advance(turn_index, carry):
        electric, magnetic, auxiliary = carry

        def electric_ahead(source, direction):
            field = electric[source]
            return forward(field, direction, zero_layer(field, direction))

        curl_h, renewed_h = curl(electric_ahead, auxiliary, 0, magnetic_coef, update_term)
        magnetic_new = jnp.stack([magnetic[component] - time_step * curl_h[component] for component in range(3)])

        def magnetic_behind(source, direction):
            field = magnetic_new[source]
            return backward(field, direction, zero_layer(field, direction))

        curl_e, renewed_e = curl(magnetic_behind, auxiliary, 6, electric_coef, update_term)
        electric_new = jnp.stack([keeping * electric[component] + driving * curl_e[component] for component in range(3)])
        return (electric_new, magnetic_new, jnp.stack(renewed_h + renewed_e))

    e_out, h_out, psi_out = lax.fori_loop(0, STEPS, advance, (e_field, h_field, psi))
    return (e_out, h_out, psi_out)
```

```python
import jax
import jax.numpy as jnp
from jax import lax
from jax.experimental import pallas as pl
from jax.experimental.pallas import tpu as pltpu
from jax.sharding import PartitionSpec as P

PML = 16
STEPS = 16
NMAT = 8
SUB = 8
GROUP = 4

time_step = 0.5
sigma_peak = 3.0
kappa_peak = 5.0
alpha_peak = 0.05
MESH = pl.DeviceIdType.MESH


def profile(index, extent, shift_half):
    position = index.astype(jnp.float32) + shift_half
    slab_width = float(PML)
    depth_frac = jnp.maximum(
        jnp.maximum(
            (slab_width - position) / slab_width, (position - (extent - slab_width)) / slab_width
        ),
        0.0,
    )
    depth_cube = depth_frac * depth_frac * depth_frac
    sigma_value = sigma_peak * depth_cube
    kappa_value = 1.0 + (kappa_peak - 1.0) * depth_cube
    alpha_value = alpha_peak * (1.0 - depth_frac)
    decays = jnp.exp(-(sigma_value / kappa_value + alpha_value) * time_step)
    scaling = (
        sigma_value * (decays - 1.0) / (kappa_value * (sigma_value + kappa_value * alpha_value))
    )
    inside_slab = depth_frac > 0.0
    return (
        jnp.where(inside_slab, decays, 0.0),
        jnp.where(inside_slab, scaling, 0.0),
        1.0 / kappa_value,
    )


def make_kernel(size_x, size_y, rows_x, rows_y, depth_z):
    groups = rows_x // GROUP
    tiles = rows_y // SUB
    top, right = rows_x - 1, rows_y - 1

    def kernel(
        e_in, h_in, p_in, m_in, eps_ref, sig_ref, e_out, h_out, p_out,
        E, H, S, keep, drive, mat, cx, cy,
        t_ex, t_ey, t_ax, t_ay, t_c0, t_c1,
        r_ex, r_ey, r_ax, r_ay, r_c0, r_c1,
        in_sem, out_sem, send_sem, recv_sem,
    ):
        gx, gy = lax.axis_index("gx"), lax.axis_index("gy")
        has_lx, has_hx = gx > 0, gx < size_x - 1
        has_ly, has_hy = gy > 0, gy < size_y - 1
        slab_x = (gx == 0, gx == size_x - 1)
        slab_y = (gy == 0, gy == size_y - 1)
        lx, hx, ly, hy = gx - 1, gx + 1, gy - 1, gy + 1
        both = jnp.logical_and
        links = (
            (has_lx, (lx, gy)),
            (has_hx, (hx, gy)),
            (has_ly, (gx, ly)),
            (has_hy, (gx, hy)),
            (both(has_hx, has_ly), (hx, ly)),
            (both(has_lx, has_hy), (lx, hy)),
        )

        plain = [
            (e_in, E.at[:, pl.ds(0, rows_x), pl.ds(0, rows_y), :]),
            (h_in, H.at[:, pl.ds(1, rows_x), pl.ds(SUB, rows_y), :]),
            (m_in, mat),
            (p_in.at[pl.ds(1, 2)], S.at[pl.ds(1, 2)]),
            (p_in.at[pl.ds(7, 2)], S.at[pl.ds(7, 2)]),
        ]
        copies = [pltpu.make_async_copy(a, b, in_sem.at[n]) for n, (a, b) in enumerate(plain)]
        for c in copies:
            c.start()

        def slab_copies(side):
            half_x = pl.ds(side * PML, PML)
            xs = [
                pltpu.make_async_copy(
                    p_in.at[pl.ds(s, 2), half_x], S.at[pl.ds(s, 2), half_x], in_sem.at[5 + n]
                )
                for n, s in enumerate((3, 9))
            ]
            ys = [
                pltpu.make_async_copy(
                    p_in.at[s, :, half_x], S.at[s, :, half_x], in_sem.at[7 + n]
                )
                for n, s in enumerate((0, 5, 6, 11))
            ]
            return xs, ys

        for side in (0, 1):
            xs, ys = slab_copies(side)

            @pl.when(slab_x[side])
            def _():
                for c in xs:
                    c.start()

            @pl.when(slab_y[side])
            def _():
                for c in ys:
                    c.start()

        for ref in (r_ex, r_ey, r_ax, r_ay, r_c0, r_c1):
            ref[...] = jnp.zeros(ref.shape, jnp.float32)

        barrier = pltpu.get_barrier_semaphore()
        for present, target in links:

            @pl.when(present)
            def _():
                pl.semaphore_signal(barrier, inc=1, device_id=target, device_id_type=MESH)

        zero = jnp.zeros((SUB, depth_z), jnp.float32)
        for side in (0, 1):

            @pl.when(jnp.logical_not(slab_x[side]))
            def _():
                @pl.loop(side * PML, side * PML + PML)
                def _(i):
                    for s in (3, 4, 9, 10):
                        S[s, i] = jnp.zeros((rows_y, depth_z), jnp.float32)

            @pl.when(jnp.logical_not(slab_y[side]))
            def _():
                @pl.loop(0, rows_x)
                def _(i):
                    for s in (0, 5, 6, 11):
                        S[s, i, pl.ds(side * PML, PML), :] = jnp.zeros(
                            (PML, depth_z), jnp.float32
                        )

        for c in range(3):
            for t in range(tiles):
                E[c, rows_x, pl.ds(t * SUB, SUB), :] = zero
                H[c, 0, pl.ds(SUB + t * SUB, SUB), :] = zero

        @pl.loop(0, rows_x)
        def _(i):
            for c in range(3):
                E[c, i, pl.ds(rows_y, SUB), :] = zero
                H[c, i + 1, pl.ds(0, SUB), :] = zero

        lane = lax.broadcasted_iota(jnp.int32, (SUB, depth_z), 1)
        row = lax.broadcasted_iota(jnp.int32, (rows_y, depth_z), 0)
        plane = lax.broadcasted_iota(jnp.int32, (rows_x, SUB, depth_z), 0)
        zc = []
        for k, shift in enumerate((0.5, 0.0)):
            zc.append(profile(lane, depth_z, shift))
            for n, v in enumerate(profile(row + gy * rows_y, size_y * rows_y, shift)):
                cy[k, n] = v
            for n, v in enumerate(profile(plane + gx * rows_x, size_x * rows_x, shift)):
                cx[k, n] = v
        not_last = lane < depth_z - 1
        not_first = lane > 0

        keep_vals, drive_vals = [], []
        for m in range(NMAT):
            eps = jnp.full((SUB, depth_z), eps_ref[m], jnp.float32)
            sig = jnp.full((SUB, depth_z), sig_ref[m], jnp.float32)
            loss = sig * time_step / (2.0 * eps)
            keep_vals.append((1.0 - loss) / (1.0 + loss))
            drive_vals.append((time_step / eps) / (1.0 + loss))
        copies[2].wait()

        @pl.loop(0, rows_x)
        def _(i):
            for t in range(tiles):
                rows = pl.ds(t * SUB, SUB)
                number = mat[i, rows, :]
                kv, dv = keep_vals[0], drive_vals[0]
                for m in range(1, NMAT):
                    chosen = number == m
                    kv = jnp.where(chosen, keep_vals[m], kv)
                    dv = jnp.where(chosen, drive_vals[m], dv)
                keep[i, rows, :] = kv
                drive[i, rows, :] = dv

        for n in (0, 1, 3, 4):
            copies[n].wait()
        for side in (0, 1):
            xs, ys = slab_copies(side)

            @pl.when(slab_x[side])
            def _():
                for c in xs:
                    c.wait()

            @pl.when(slab_y[side])
            def _():
                for c in ys:
                    c.wait()

        pl.semaphore_wait(barrier, sum(jnp.where(present, 1, 0) for present, _t in links))

        def term(slot, i, rows, d, coef):
            b, a, q = coef
            renewed = b * S[slot, i, rows, :] + a * d
            S[slot, i, rows, :] = renewed
            return q * d + renewed

        def h_tile(i, y, in_x, in_y):
            rows = pl.ds(y, SUB)
            e0, e1, e2 = (E[c, i, rows, :] for c in range(3))
            dx1 = E[1, i + 1, rows, :] - e1
            dx2 = E[2, i + 1, rows, :] - e2
            nxt = pl.ds(y + 1, SUB)
            dy0 = E[0, i, nxt, :] - e0
            dy2 = E[2, i, nxt, :] - e2
            dz0 = jnp.where(not_last, pltpu.roll(e0, depth_z - 1, 1), 0.0) - e0
            dz1 = jnp.where(not_last, pltpu.roll(e1, depth_z - 1, 1), 0.0) - e1
            t1 = term(1, i, rows, dz1, zc[0])
            t2 = term(2, i, rows, dz0, zc[0])
            if in_x:
                coef = tuple(cx[0, n, i] for n in range(3))
                dx2 = term(3, i, rows, dx2, coef)
                dx1 = term(4, i, rows, dx1, coef)
            if in_y:
                coef = tuple(cy[0, n, rows, :] for n in range(3))
                dy2 = term(0, i, rows, dy2, coef)
                dy0 = term(5, i, rows, dy0, coef)
            out = pl.ds(y + SUB, SUB)
            H[0, i + 1, out, :] = H[0, i + 1, out, :] - time_step * (dy2 - t1)
            H[1, i + 1, out, :] = H[1, i + 1, out, :] - time_step * (t2 - dx2)
            H[2, i + 1, out, :] = H[2, i + 1, out, :] - time_step * (dx1 - dy0)

        def e_tile(i, y, in_x, in_y):
            rows = pl.ds(y, SUB)
            at = pl.ds(y + SUB, SUB)
            prv = pl.ds(y + SUB - 1, SUB)
            h0, h1, h2 = (H[c, i + 1, at, :] for c in range(3))
            dx1 = h1 - H[1, i, at, :]
            dx2 = h2 - H[2, i, at, :]
            dy0 = h0 - H[0, i + 1, prv, :]
            dy2 = h2 - H[2, i + 1, prv, :]
            dz0 = h0 - jnp.where(not_first, pltpu.roll(h0, 1, 1), 0.0)
            dz1 = h1 - jnp.where(not_first, pltpu.roll(h1, 1, 1), 0.0)
            t7 = term(7, i, rows, dz1, zc[1])
            t8 = term(8, i, rows, dz0, zc[1])
            if in_x:
                coef = tuple(cx[1, n, i] for n in range(3))
                dx2 = term(9, i, rows, dx2, coef)
                dx1 = term(10, i, rows, dx1, coef)
            if in_y:
                coef = tuple(cy[1, n, rows, :] for n in range(3))
                dy2 = term(6, i, rows, dy2, coef)
                dy0 = term(11, i, rows, dy0, coef)
            k, d = keep[i, rows, :], drive[i, rows, :]
            E[0, i, rows, :] = k * E[0, i, rows, :] + d * (dy2 - t7)
            E[1, i, rows, :] = k * E[1, i, rows, :] + d * (t8 - dx2)
            E[2, i, rows, :] = k * E[2, i, rows, :] + d * (dx1 - dy0)

        def unit(tile_fn, g, t):
            low_x, low_y = g * GROUP < PML, t * SUB < PML
            px = jnp.where(low_x, slab_x[0], slab_x[1])
            py = jnp.where(low_y, slab_y[0], slab_y[1])
            y = pl.multiple_of(t * SUB, SUB)
            for in_x in (False, True):
                for in_y in (False, True):

                    @pl.when(both(px == in_x, py == in_y))
                    def _():
                        for u in range(GROUP):
                            tile_fn(g * GROUP + u, y, in_x, in_y)

        def exchange(s):
            moves = (
                (has_lx, (lx, gy), has_hx, t_ex, r_ex),
                (has_ly, (gx, ly), has_hy, t_ey, r_ey),
                (both(has_hx, has_ly), (hx, ly), both(has_lx, has_hy), t_c0, r_c0),
                (both(has_lx, has_hy), (lx, hy), both(has_hx, has_ly), t_c1, r_c1),
                (has_hx, (hx, gy), has_lx, t_ax, r_ax),
                (has_hy, (gx, hy), has_ly, t_ay, r_ay),
            )
            return [
                (
                    sends,
                    gets,
                    pltpu.make_async_remote_copy(
                        src_ref=src,
                        dst_ref=dst.at[s],
                        send_sem=send_sem.at[n],
                        recv_sem=recv_sem.at[n, s],
                        device_id=target,
                        device_id_type=MESH,
                    ),
                )
                for n, (sends, target, gets, src, dst) in enumerate(moves)
            ]

        own = pl.ds(0, rows_y)
        inner = pl.ds(SUB, rows_y)

        def advance(step, carry):
            s = lax.rem(step, 2)
            moves = exchange(s)
            t_ex[0] = E[1, 0, own, :]
            t_ex[1] = E[2, 0, own, :]
            t_c0[...] = E[0, top, pl.ds(0, SUB), :]
            t_c1[...] = E[1, 0, pl.ds(rows_y - SUB, SUB), :]
            for i in range(rows_x):
                t_ey[0, pl.ds(i, 1), :] = E[0, i, pl.ds(0, 1), :]
                t_ey[1, pl.ds(i, 1), :] = E[2, i, pl.ds(0, 1), :]
            for sends, _g, copy in moves[:4]:

                @pl.when(sends)
                def _():
                    copy.start()

            @pl.loop(0, tiles + groups - 1)
            def _(k):
                face = k < tiles
                unit(
                    h_tile, jnp.where(face, groups - 1, k - tiles), jnp.where(face, k, tiles - 1)
                )

            t_ax[0] = H[1, rows_x, inner, :]
            t_ax[1] = H[2, rows_x, inner, :]
            for i in range(rows_x):
                t_ay[0, pl.ds(i, 1), :] = H[0, i + 1, pl.ds(SUB + right, 1), :]
                t_ay[1, pl.ds(i, 1), :] = H[2, i + 1, pl.ds(SUB + right, 1), :]
            for sends, _g, copy in moves[4:]:

                @pl.when(sends)
                def _():
                    copy.start()

            @pl.loop(0, (groups - 1) * (tiles - 1))
            def _(k):
                unit(h_tile, lax.div(k, tiles - 1), lax.rem(k, tiles - 1))

            @pl.loop(0, (groups - 2) * (tiles - 2))
            def _(k):
                unit(e_tile, 1 + lax.div(k, tiles - 2), 1 + lax.rem(k, tiles - 2))

            for _s, gets, copy in moves:

                @pl.when(gets)
                def _():
                    copy.wait_recv()

            half = time_step

            @pl.when(has_hx)
            def _():
                H[1, rows_x, inner, :] = H[1, rows_x, inner, :] + half * r_ex[s, 1]
                H[2, rows_x, inner, :] = H[2, rows_x, inner, :] - half * r_ex[s, 0]

            @pl.when(has_hy)
            def _():
                edge = pl.ds(SUB + right, 1)
                for i in range(rows_x):
                    H[0, i + 1, edge, :] = (
                        H[0, i + 1, edge, :] - half * r_ey[s, 1, pl.ds(i, 1), :]
                    )
                    H[2, i + 1, edge, :] = (
                        H[2, i + 1, edge, :] + half * r_ey[s, 0, pl.ds(i, 1), :]
                    )

            @pl.when(has_lx)
            def _():
                H[1, 0, inner, :] = r_ax[s, 0] + half * E[2, 0, own, :]
                H[2, 0, inner, :] = r_ax[s, 1] - half * E[1, 0, own, :]
                edge = pl.ds(SUB + right, 1)
                H[2, 0, edge, :] = H[2, 0, edge, :] + half * r_c0[s, pl.ds(0, 1), :]

            @pl.when(has_ly)
            def _():
                edge = pl.ds(SUB - 1, 1)
                first = pl.ds(0, 1)
                for i in range(rows_x):
                    line = pl.ds(i, 1)
                    H[0, i + 1, edge, :] = r_ay[s, 0, line, :] - half * E[2, i, first, :]
                    H[2, i + 1, edge, :] = r_ay[s, 1, line, :] + half * E[0, i, first, :]
                H[2, rows_x, edge, :] = (
                    H[2, rows_x, edge, :] - half * r_c1[s, pl.ds(SUB - 1, 1), :]
                )

            @pl.loop(0, 2 * groups + 2 * (tiles - 2))
            def _(k):
                side = k < 2 * groups
                j = k - 2 * groups
                g = jnp.where(side, lax.rem(k, groups), (groups - 1) * lax.rem(j, 2))
                t = jnp.where(side, (tiles - 1) * lax.div(k, groups), 1 + lax.div(j, 2))
                unit(e_tile, g, t)

            for sends, _g, copy in moves:

                @pl.when(sends)
                def _():
                    copy.wait_send()

            return carry

        lax.fori_loop(0, STEPS, advance, 0)

        outs = [
            pltpu.make_async_copy(
                E.at[:, pl.ds(0, rows_x), pl.ds(0, rows_y), :], e_out, out_sem.at[0]
            ),
            pltpu.make_async_copy(
                H.at[:, pl.ds(1, rows_x), pl.ds(SUB, rows_y), :], h_out, out_sem.at[1]
            ),
            pltpu.make_async_copy(S, p_out, out_sem.at[2]),
        ]
        for c in outs:
            c.start()
        for c in outs:
            c.wait()

    return kernel


def solution(mesh):
    size_x, size_y = mesh.shape["gx"], mesh.shape["gy"]

    def shards(e_field, h_field, psi, material, eps_table, sigma_table):
        _, rows_x, rows_y, depth_z = e_field.shape
        assert rows_x == 2 * PML and rows_y == 2 * PML and size_x > 1 and size_y > 1
        f32 = jnp.float32
        any_space = pl.BlockSpec(memory_space=pl.ANY)
        smem = pl.BlockSpec(memory_space=pltpu.SMEM)
        face_x = (2, rows_y, depth_z)
        face_y = (2, rows_x, depth_z)
        corner = (SUB, depth_z)
        faces = (face_x, face_y, face_x, face_y, corner, corner)
        padded = (3, rows_x + 1, rows_y + SUB, depth_z)
        cell = (rows_x, rows_y, depth_z)
        return pl.pallas_call(
            make_kernel(size_x, size_y, rows_x, rows_y, depth_z),
            out_shape=[jax.ShapeDtypeStruct(a.shape, f32) for a in (e_field, h_field, psi)],
            in_specs=[any_space] * 4 + [smem] * 2,
            out_specs=[any_space] * 3,
            scratch_shapes=[
                pltpu.VMEM(padded, f32),
                pltpu.VMEM(padded, f32),
                pltpu.VMEM(psi.shape, f32),
                pltpu.VMEM(cell, f32),
                pltpu.VMEM(cell, f32),
                pltpu.VMEM(cell, jnp.int32),
                pltpu.VMEM((2, 3, rows_x, SUB, depth_z), f32),
                pltpu.VMEM((2, 3, rows_y, depth_z), f32),
            ]
            + [pltpu.VMEM(f, f32) for f in faces]
            + [pltpu.VMEM((2,) + f, f32) for f in faces]
            + [
                pltpu.SemaphoreType.DMA((11,)),
                pltpu.SemaphoreType.DMA((3,)),
                pltpu.SemaphoreType.DMA((6,)),
                pltpu.SemaphoreType.DMA((6, 2)),
            ],
            compiler_params=pltpu.CompilerParams(collective_id=0, has_side_effects=True),
        )(e_field, h_field, psi, material, eps_table, sigma_table)

    split = P(None, "gx", "gy", None)
    return jax.shard_map(
        shards,
        mesh=mesh,
        in_specs=(split, split, split, P("gx", "gy", None), P(), P()),
        out_specs=(split, split, split),
        check_vma=False,
    )
```

```python
import jax
import jax.numpy as jnp
from jax import lax
from jax.experimental import pallas as pl
from jax.experimental.pallas import tpu as pltpu
from jax.sharding import PartitionSpec as P

PML = 16
STEPS = 16
NMAT = 8
SUB = 8
GROUP = 16
AHEAD = 2

time_step = 0.5
sigma_peak = 3.0
kappa_peak = 5.0
alpha_peak = 0.05
MESH = pl.DeviceIdType.MESH


def profile(index, extent, shift_half):
    position = index.astype(jnp.float32) + shift_half
    slab_width = float(PML)
    depth_frac = jnp.maximum(
        jnp.maximum(
            (slab_width - position) / slab_width, (position - (extent - slab_width)) / slab_width
        ),
        0.0,
    )
    depth_cube = depth_frac * depth_frac * depth_frac
    sigma_value = sigma_peak * depth_cube
    kappa_value = 1.0 + (kappa_peak - 1.0) * depth_cube
    alpha_value = alpha_peak * (1.0 - depth_frac)
    decays = jnp.exp(-(sigma_value / kappa_value + alpha_value) * time_step)
    scaling = (
        sigma_value * (decays - 1.0) / (kappa_value * (sigma_value + kappa_value * alpha_value))
    )
    inside_slab = depth_frac > 0.0
    return (
        jnp.where(inside_slab, decays, 0.0),
        jnp.where(inside_slab, scaling, 0.0),
        1.0 / kappa_value,
    )


def make_kernel(size_x, size_y, rows_x, rows_y, depth_z):
    groups = rows_x // GROUP
    tiles = rows_y // SUB
    top, right = rows_x - 1, rows_y - 1

    def kernel(
        e_in, h_in, p_in, m_in, eps_ref, sig_ref, E, H, S,
        keep, drive, mat, cx, cy,
        t_ex, t_ey, t_ax, t_ay, t_c0, t_c1,
        r_ex, r_ey, r_ax, r_ay, r_c0, r_c1,
        in_sem, send_sem, recv_sem,
    ):
        gx, gy = lax.axis_index("gx"), lax.axis_index("gy")
        has_lx, has_hx = gx > 0, gx < size_x - 1
        has_ly, has_hy = gy > 0, gy < size_y - 1
        slab_x = (gx == 0, gx == size_x - 1)
        slab_y = (gy == 0, gy == size_y - 1)
        lx, hx, ly, hy = gx - 1, gx + 1, gy - 1, gy + 1
        both = jnp.logical_and
        links = (
            (has_lx, (lx, gy)),
            (has_hx, (hx, gy)),
            (has_ly, (gx, ly)),
            (has_hy, (gx, hy)),
            (both(has_hx, has_ly), (hx, ly)),
            (both(has_lx, has_hy), (lx, hy)),
        )

        plain = [
            (e_in, E.at[:, pl.ds(0, rows_x), pl.ds(0, rows_y), :]),
            (h_in, H.at[:, pl.ds(1, rows_x), pl.ds(SUB, rows_y), :]),
            (m_in, mat),
            (p_in.at[pl.ds(1, 2)], S.at[pl.ds(1, 2)]),
            (p_in.at[pl.ds(7, 2)], S.at[pl.ds(7, 2)]),
        ]
        copies = [pltpu.make_async_copy(a, b, in_sem.at[n]) for n, (a, b) in enumerate(plain)]
        for c in copies:
            c.start()

        def slab_copies(side):
            half_x = pl.ds(side * PML, PML)
            xs = [
                pltpu.make_async_copy(
                    p_in.at[pl.ds(s, 2), half_x], S.at[pl.ds(s, 2), half_x], in_sem.at[5 + n]
                )
                for n, s in enumerate((3, 9))
            ]
            ys = [
                pltpu.make_async_copy(
                    p_in.at[s, :, half_x], S.at[s, :, half_x], in_sem.at[7 + n]
                )
                for n, s in enumerate((0, 5, 6, 11))
            ]
            return xs, ys

        for side in (0, 1):
            xs, ys = slab_copies(side)

            @pl.when(slab_x[side])
            def _():
                for c in xs:
                    c.start()

            @pl.when(slab_y[side])
            def _():
                for c in ys:
                    c.start()

        for ref in (r_ex, r_ey, r_ax, r_ay, r_c0, r_c1):
            ref[...] = jnp.zeros(ref.shape, jnp.float32)

        barrier = pltpu.get_barrier_semaphore()
        for present, target in links:

            @pl.when(present)
            def _():
                pl.semaphore_signal(barrier, inc=1, device_id=target, device_id_type=MESH)

        zero = jnp.zeros((SUB, depth_z), jnp.float32)
        for side in (0, 1):

            @pl.when(jnp.logical_not(slab_x[side]))
            def _():
                @pl.loop(side * PML, side * PML + PML)
                def _(i):
                    for s in (3, 4, 9, 10):
                        S[s, i] = jnp.zeros((rows_y, depth_z), jnp.float32)

            @pl.when(jnp.logical_not(slab_y[side]))
            def _():
                @pl.loop(0, rows_x)
                def _(i):
                    for s in (0, 5, 6, 11):
                        S[s, i, pl.ds(side * PML, PML), :] = jnp.zeros(
                            (PML, depth_z), jnp.float32
                        )

        for c in range(3):
            for t in range(tiles):
                E[c, rows_x, pl.ds(t * SUB, SUB), :] = zero
                H[c, 0, pl.ds(SUB + t * SUB, SUB), :] = zero

        @pl.loop(0, rows_x)
        def _(i):
            for c in range(3):
                E[c, i, pl.ds(rows_y, SUB), :] = zero
                H[c, i + 1, pl.ds(0, SUB), :] = zero

        lane = lax.broadcasted_iota(jnp.int32, (SUB, depth_z), 1)
        row = lax.broadcasted_iota(jnp.int32, (rows_y, depth_z), 0)
        plane = lax.broadcasted_iota(jnp.int32, (rows_x, SUB, depth_z), 0)
        zc = []
        for k, shift in enumerate((0.5, 0.0)):
            zc.append(profile(lane, depth_z, shift))
            for n, v in enumerate(profile(row + gy * rows_y, size_y * rows_y, shift)):
                cy[k, n] = v
            for n, v in enumerate(profile(plane + gx * rows_x, size_x * rows_x, shift)):
                cx[k, n] = v
        not_last = lane < depth_z - 1
        not_first = lane > 0

        keep_vals, drive_vals = [], []
        for m in range(NMAT):
            eps = jnp.full((SUB, depth_z), eps_ref[m], jnp.float32)
            sig = jnp.full((SUB, depth_z), sig_ref[m], jnp.float32)
            loss = sig * time_step / (2.0 * eps)
            keep_vals.append((1.0 - loss) / (1.0 + loss))
            drive_vals.append((time_step / eps) / (1.0 + loss))
        copies[2].wait()

        @pl.loop(0, rows_x)
        def _(i):
            for t in range(tiles):
                rows = pl.ds(t * SUB, SUB)
                number = mat[i, rows, :]
                kv, dv = keep_vals[0], drive_vals[0]
                for m in range(1, NMAT):
                    chosen = number == m
                    kv = jnp.where(chosen, keep_vals[m], kv)
                    dv = jnp.where(chosen, drive_vals[m], dv)
                keep[i, rows, :] = kv
                drive[i, rows, :] = dv

        for n in (0, 1, 3, 4):
            copies[n].wait()
        for side in (0, 1):
            xs, ys = slab_copies(side)

            @pl.when(slab_x[side])
            def _():
                for c in xs:
                    c.wait()

            @pl.when(slab_y[side])
            def _():
                for c in ys:
                    c.wait()

        pl.semaphore_wait(barrier, sum(jnp.where(present, 1, 0) for present, _t in links))

        def term(old, d, coef):
            b, a, q = coef
            renewed = b * old + a * d
            return q * d + renewed, renewed

        def loads(k, i, y, in_x, in_y):
            rows, at = pl.ds(y, SUB), pl.ds(y + SUB, SUB)
            first = 6 * k
            if k == 0:
                src, j, now, step, line = E, i, rows, 1, pl.ds(y + 1, SUB)
                old = [H[c, i + 1, at, :] for c in range(3)]
                mats = ()
            else:
                src, j, now, step, line = H, i + 1, at, -1, pl.ds(y + SUB - 1, SUB)
                old = [E[c, i, rows, :] for c in range(3)]
                mats = (keep[i, rows, :], drive[i, rows, :])
            own = [src[c, j, now, :] for c in range(3)]
            side_x = [src[c, j + step, now, :] for c in (1, 2)]
            side_y = [src[c, j, line, :] for c in (0, 2)]
            slots = [1, 2] + ([3, 4] if in_x else []) + ([0, 5] if in_y else [])
            aux = {n: S[first + n, i, rows, :] for n in slots}
            coef_x = [cx[k, n, i] for n in range(3)] if in_x else None
            return own, side_x, side_y, old, mats, aux, coef_x

        def compute(k, values, coef_y):
            own, (x1, x2), (y0, y2), old, mats, aux, coef_x = values
            f0, f1, f2 = own
            if k == 0:
                dx1, dx2, dy0, dy2 = x1 - f1, x2 - f2, y0 - f0, y2 - f2
                dz0 = jnp.where(not_last, pltpu.roll(f0, depth_z - 1, 1), 0.0) - f0
                dz1 = jnp.where(not_last, pltpu.roll(f1, depth_z - 1, 1), 0.0) - f1
            else:
                dx1, dx2, dy0, dy2 = f1 - x1, f2 - x2, f0 - y0, f2 - y2
                dz0 = f0 - jnp.where(not_first, pltpu.roll(f0, 1, 1), 0.0)
                dz1 = f1 - jnp.where(not_first, pltpu.roll(f1, 1, 1), 0.0)
            fresh = {}
            dz1, fresh[1] = term(aux[1], dz1, zc[k])
            dz0, fresh[2] = term(aux[2], dz0, zc[k])
            if coef_x is not None:
                dx2, fresh[3] = term(aux[3], dx2, coef_x)
                dx1, fresh[4] = term(aux[4], dx1, coef_x)
            if coef_y is not None:
                dy2, fresh[0] = term(aux[0], dy2, coef_y)
                dy0, fresh[5] = term(aux[5], dy0, coef_y)
            curls = (dy2 - dz1, dz0 - dx2, dx1 - dy0)
            if k == 0:
                return [o - time_step * c for o, c in zip(old, curls)], fresh
            return [mats[0] * o + mats[1] * c for o, c in zip(old, curls)], fresh

        def stores(k, i, y, result):
            fields, fresh = result
            for c in range(3):
                if k == 0:
                    H[c, i + 1, pl.ds(y + SUB, SUB), :] = fields[c]
                else:
                    E[c, i, pl.ds(y, SUB), :] = fields[c]
            for n, v in fresh.items():
                S[6 * k + n, i, pl.ds(y, SUB), :] = v

        def run(k, i0, y, in_x, in_y):
            coef_y = [cy[k, n, pl.ds(y, SUB), :] for n in range(3)] if in_y else None
            ready = [loads(k, i0 + u, y, in_x, in_y) for u in range(AHEAD)]
            for u in range(GROUP):
                if u + AHEAD < GROUP:
                    ready.append(loads(k, i0 + u + AHEAD, y, in_x, in_y))
                stores(k, i0 + u, y, compute(k, ready[u], coef_y))

        def unit(k, g, t):
            low_x, low_y = g * GROUP < PML, t * SUB < PML
            px = jnp.where(low_x, slab_x[0], slab_x[1])
            py = jnp.where(low_y, slab_y[0], slab_y[1])
            i0, y = g * GROUP, pl.multiple_of(t * SUB, SUB)

            def split_y(in_x):
                lax.cond(
                    py,
                    lambda: run(k, i0, y, in_x, True),
                    lambda: run(k, i0, y, in_x, False),
                )

            lax.cond(px, lambda: split_y(True), lambda: split_y(False))

        def exchange(s):
            moves = (
                (has_lx, (lx, gy), has_hx, t_ex, r_ex),
                (has_ly, (gx, ly), has_hy, t_ey, r_ey),
                (both(has_hx, has_ly), (hx, ly), both(has_lx, has_hy), t_c0, r_c0),
                (both(has_lx, has_hy), (lx, hy), both(has_hx, has_ly), t_c1, r_c1),
                (has_hx, (hx, gy), has_lx, t_ax, r_ax),
                (has_hy, (gx, hy), has_ly, t_ay, r_ay),
            )
            return [
                (
                    sends,
                    gets,
                    pltpu.make_async_remote_copy(
                        src_ref=src,
                        dst_ref=dst.at[s],
                        send_sem=send_sem.at[n],
                        recv_sem=recv_sem.at[n, s],
                        device_id=target,
                        device_id_type=MESH,
                    ),
                )
                for n, (sends, target, gets, src, dst) in enumerate(moves)
            ]

        own = pl.ds(0, rows_y)
        inner = pl.ds(SUB, rows_y)

        def advance(step, carry):
            s = lax.rem(step, 2)
            moves = exchange(s)
            t_ex[0] = E[1, 0, own, :]
            t_ex[1] = E[2, 0, own, :]
            t_c0[...] = E[0, top, pl.ds(0, SUB), :]
            t_c1[...] = E[1, 0, pl.ds(rows_y - SUB, SUB), :]
            for i in range(rows_x):
                t_ey[0, pl.ds(i, 1), :] = E[0, i, pl.ds(0, 1), :]
                t_ey[1, pl.ds(i, 1), :] = E[2, i, pl.ds(0, 1), :]
            for sends, _g, copy in moves[:4]:

                @pl.when(sends)
                def _():
                    copy.start()

            @pl.loop(0, tiles + groups - 1)
            def _(k):
                face = k < tiles
                unit(
                    0, jnp.where(face, groups - 1, k - tiles), jnp.where(face, k, tiles - 1)
                )

            t_ax[0] = H[1, rows_x, inner, :]
            t_ax[1] = H[2, rows_x, inner, :]
            for i in range(rows_x):
                t_ay[0, pl.ds(i, 1), :] = H[0, i + 1, pl.ds(SUB + right, 1), :]
                t_ay[1, pl.ds(i, 1), :] = H[2, i + 1, pl.ds(SUB + right, 1), :]
            for sends, _g, copy in moves[4:]:

                @pl.when(sends)
                def _():
                    copy.start()

            @pl.loop(0, (groups - 1) * (tiles - 1))
            def _(k):
                unit(0, lax.div(k, tiles - 1), lax.rem(k, tiles - 1))

            @pl.loop(0, (groups - 2) * (tiles - 2))
            def _(k):
                unit(1, 1 + lax.div(k, tiles - 2), 1 + lax.rem(k, tiles - 2))

            for _s, gets, copy in moves:

                @pl.when(gets)
                def _():
                    copy.wait_recv()

            half = time_step

            @pl.when(has_hx)
            def _():
                H[1, rows_x, inner, :] = H[1, rows_x, inner, :] + half * r_ex[s, 1]
                H[2, rows_x, inner, :] = H[2, rows_x, inner, :] - half * r_ex[s, 0]

            @pl.when(has_hy)
            def _():
                edge = pl.ds(SUB + right, 1)
                for i in range(rows_x):
                    H[0, i + 1, edge, :] = (
                        H[0, i + 1, edge, :] - half * r_ey[s, 1, pl.ds(i, 1), :]
                    )
                    H[2, i + 1, edge, :] = (
                        H[2, i + 1, edge, :] + half * r_ey[s, 0, pl.ds(i, 1), :]
                    )

            @pl.when(has_lx)
            def _():
                H[1, 0, inner, :] = r_ax[s, 0] + half * E[2, 0, own, :]
                H[2, 0, inner, :] = r_ax[s, 1] - half * E[1, 0, own, :]
                edge = pl.ds(SUB + right, 1)
                H[2, 0, edge, :] = H[2, 0, edge, :] + half * r_c0[s, pl.ds(0, 1), :]

            @pl.when(has_ly)
            def _():
                edge = pl.ds(SUB - 1, 1)
                first = pl.ds(0, 1)
                for i in range(rows_x):
                    line = pl.ds(i, 1)
                    H[0, i + 1, edge, :] = r_ay[s, 0, line, :] - half * E[2, i, first, :]
                    H[2, i + 1, edge, :] = r_ay[s, 1, line, :] + half * E[0, i, first, :]
                H[2, rows_x, edge, :] = (
                    H[2, rows_x, edge, :] - half * r_c1[s, pl.ds(SUB - 1, 1), :]
                )

            @pl.loop(0, 2 * groups + 2 * (tiles - 2))
            def _(k):
                side = k < 2 * groups
                j = k - 2 * groups
                g = jnp.where(side, lax.rem(k, groups), (groups - 1) * lax.rem(j, 2))
                t = jnp.where(side, (tiles - 1) * lax.div(k, groups), 1 + lax.div(j, 2))
                unit(1, g, t)

            for sends, _g, copy in moves:

                @pl.when(sends)
                def _():
                    copy.wait_send()

            return carry

        lax.fori_loop(0, STEPS, advance, 0)

    return kernel


def make_writer(rows_x, rows_y):
    def writer(E, H, S, e_out, h_out, p_out, out_sem):
        outs = [
            pltpu.make_async_copy(
                E.at[:, pl.ds(0, rows_x), pl.ds(0, rows_y), :], e_out, out_sem.at[0]
            ),
            pltpu.make_async_copy(
                H.at[:, pl.ds(1, rows_x), pl.ds(SUB, rows_y), :], h_out, out_sem.at[1]
            ),
            pltpu.make_async_copy(S, p_out, out_sem.at[2]),
        ]
        for c in outs:
            c.start()
        for c in outs:
            c.wait()

    return writer


def solution(mesh):
    size_x, size_y = mesh.shape["gx"], mesh.shape["gy"]

    def shards(e_field, h_field, psi, material, eps_table, sigma_table):
        _, rows_x, rows_y, depth_z = e_field.shape
        assert rows_x == 2 * PML and rows_y == 2 * PML and size_x > 1 and size_y > 1
        f32 = jnp.float32
        any_space = pl.BlockSpec(memory_space=pltpu.HBM)
        smem = pl.BlockSpec(memory_space=pltpu.SMEM)
        face_x = (2, rows_y, depth_z)
        face_y = (2, rows_x, depth_z)
        corner = (SUB, depth_z)
        faces = (face_x, face_y, face_x, face_y, corner, corner)
        padded = (3, rows_x + 1, rows_y + SUB, depth_z)
        cell = (rows_x, rows_y, depth_z)
        vmem = pl.BlockSpec(memory_space=pltpu.VMEM)
        state = pl.pallas_call(
            make_kernel(size_x, size_y, rows_x, rows_y, depth_z),
            out_shape=[pltpu.VMEM(padded, f32), pltpu.VMEM(padded, f32), pltpu.VMEM(psi.shape, f32)],
            in_specs=[any_space] * 4 + [smem] * 2,
            out_specs=[vmem] * 3,
            scratch_shapes=[
                pltpu.VMEM(cell, f32),
                pltpu.VMEM(cell, f32),
                pltpu.VMEM(cell, jnp.int32),
                pltpu.VMEM((2, 3, rows_x, SUB, depth_z), f32),
                pltpu.VMEM((2, 3, rows_y, depth_z), f32),
            ]
            + [pltpu.VMEM(f, f32) for f in faces]
            + [pltpu.VMEM((2,) + f, f32) for f in faces]
            + [
                pltpu.SemaphoreType.DMA((11,)),
                pltpu.SemaphoreType.DMA((6,)),
                pltpu.SemaphoreType.DMA((6, 2)),
            ],
            compiler_params=pltpu.CompilerParams(
                collective_id=0, has_side_effects=True, vmem_limit_bytes=53 << 20
            ),
        )(e_field, h_field, psi, material, eps_table, sigma_table)
        return pl.pallas_call(
            make_writer(rows_x, rows_y),
            out_shape=[jax.ShapeDtypeStruct(a.shape, f32) for a in (e_field, h_field, psi)],
            in_specs=[vmem] * 3,
            out_specs=[any_space] * 3,
            scratch_shapes=[pltpu.SemaphoreType.DMA((3,))],
            compiler_params=pltpu.CompilerParams(vmem_limit_bytes=24 << 20),
        )(*state)

    split = P(None, "gx", "gy", None)
    return jax.shard_map(
        shards,
        mesh=mesh,
        in_specs=(split, split, split, P("gx", "gy", None), P(), P()),
        out_specs=(split, split, split),
        check_vma=False,
    )
```
